32 devices in a mesh: groups: 2 (over x), seq: 8 (over z, y), batch: 2 (over core).
Axes of the slice: x: 2, y: 2, z: 4, core: 2. Of those that a mesh axis runs over, the one named last changes fastest.
Arguments:
- prompt_cache: bfloat16 [16, 256, 8, 256], P(('groups', 'batch'), 'seq'), parts along dimension 0, may hold values from -6 to 6
- prompt_states: float32 [16, 8, 16, 16384], P(('groups', 'batch'), 'seq'), parts along dimension 0, may hold values from -6 to 6
- block_steps: float32 [16, 8, 16384], P(('groups', 'batch'), 'seq'), parts along dimension 0, may hold values from 0.005 to 0.1
- prompt_lengths: int32 [16], P('groups'), parts along dimension 0, may hold values from 42 to 255
- target_slots: int32 [16], P('groups'), parts along dimension 0, may hold values from 0 to 15, as said below
- cache_lengths: int32 [32], P(('groups', 'batch')), parts along dimension 0, may hold values from 42 to 255
- resident_cache: bfloat16 [32, 32, 8, 8, 256], P(('groups', 'batch'), None, 'seq'), parts along dimension 0, may hold values from -6 to 6
- token_cache: bfloat16 [32, 8, 256], P(('groups', 'batch')), parts along dimension 0, may hold values from -6 to 6
- queries: bfloat16 [32, 64, 128], P(('groups', 'batch')), parts along dimension 0, may hold values from -6 to 6
- resident_states: float32 [32, 16, 16384], P(('groups', 'batch'), None, 'seq'), parts along dimension 0, may hold values from -6 to 6
- decay_rates: float32 [16, 16384], replicated, may hold values from 0.05 to 10
- step_sizes: float32 [32, 16384], P(('groups', 'batch'), 'seq'), parts along dimension 0, may hold values from 0.01 to 1
- inner_input: bfloat16 [32, 16384], P(('groups', 'batch'), 'seq'), parts along dimension 0, may hold values from -6 to 6
- inner_gate: bfloat16 [32, 16384], P(('groups', 'batch'), 'seq'), parts along dimension 0, may hold values from -6 to 6
- state_input: float32 [32, 16], P(('groups', 'batch')), parts along dimension 0, may hold values from -6 to 6
- state_readout: float32 [32, 16], P(('groups', 'batch')), parts along dimension 0, may hold values from -6 to 6
- skip_gain: float32 [16384], P('seq'), may hold values from 0.5 to 1.5
Outputs:
- merged_cache: bfloat16 [32, 32, 8, 8, 256], P(('groups', 'batch'), None, 'seq'), parts along dimension 0
- attention: bfloat16 [32, 64, 128], P(('groups', 'batch'), 'seq'), parts along dimension 0
- next_states: float32 [32, 16, 16384], P(('groups', 'batch'), None, 'seq'), parts along dimension 0
- mamba_output: bfloat16 [32, 16384], P(('groups', 'batch'), 'seq'), parts along dimension 0
The draws below stay inside these ranges and needn't reach their ends.
There are 2 independent parts, one for each index of `groups`. The reference program is written for one: setup_inputs(seed, part) draws one part's arguments, and reference() takes and returns one part's arrays. A program takes and returns all parts, laid end to end along the dimension named above; an argument that names none is the same for every part. Nothing has to cross between parts.
Inputs may be any that keep to these rules, and one draw needn't show every extreme that they name: `target_slots`: 8 distinct slots.
All inputs are finite; a program needn't handle non-finite values.
Results may differ from the reference program's by a relative error of at most 0.0019.
Values may be sent and summed in bfloat16 or wider, within the bound.
A program may use at most 320 MiB of HBM per device.

```python
import math
import jax
import jax.numpy as jnp
from jax import lax

HEADS = 64
KV_HEADS = 8
HEAD_DIM = 128
INNER = 16384
STATE = 16
PROMPTS = 8
BLOCK_LEN = 32
SLOTS_DEV = 8
PROMPT_MAX = 256
SLOTS = 16
N_SEQ = 8
N_BATCH = 2


def draw_target_slots(key, part):
    shuffled = jax.random.permutation(key, SLOTS)
    return shuffled[:PROMPTS].astype(jnp.int32)


def sign_direction(key):
    return jax.random.rademacher(jax.random.fold_in(key, 7101), (KV_HEADS, HEAD_DIM), dtype=jnp.float32)


def key_amplitudes():
    return jnp.array([4.8, 4.76, 4.72], jnp.float32)


def keyed_cache(key, row_count, salt_value, level_set):
    kv_width = 2 * HEAD_DIM
    noise_key, spot_key, fine_key = jax.random.split(jax.random.fold_in(key, salt_value), 3)
    base_draw = jnp.clip(jax.random.normal(noise_key, (row_count, PROMPT_MAX, KV_HEADS, kv_width), jnp.float32), -6.0, 6.0)
    reach_len = max(PROMPT_MAX // 6, 3)

    def pick_spots(row_index):
        return jax.random.permutation(jax.random.fold_in(spot_key, row_index), reach_len)[:3].astype(jnp.int32)
    spot_rows = jax.vmap(pick_spots)(jnp.arange(row_count, dtype=jnp.int32))
    position = jnp.arange(PROMPT_MAX, dtype=jnp.int32)
    hit_table = (position[None, None, :] == spot_rows[:, :, None]).astype(jnp.float32)
    amplitude = jnp.einsum('rkt,k->rt', hit_table, level_set)
    chosen = jnp.sum(hit_table, axis=1)
    direction = sign_direction(key)
    fine_noise = 0.02 * jnp.clip(jax.random.normal(fine_key, (row_count, PROMPT_MAX, KV_HEADS, HEAD_DIM), jnp.float32), -3.0, 3.0)
    aligned = amplitude[:, :, None, None] * direction[None, None] + fine_noise
    new_keys = jnp.where(chosen[:, :, None, None] > 0.5, aligned, base_draw[..., :HEAD_DIM])
    return jnp.concatenate([new_keys, base_draw[..., HEAD_DIM:]], axis=3)


def draw_prompt_cache(key, part):
    level_set = key_amplitudes()
    return keyed_cache(key, PROMPTS, 11, level_set).astype(jnp.bfloat16)


def draw_resident_cache(key, part):
    level_set = key_amplitudes()
    filled = keyed_cache(key, SLOTS, 13, level_set)
    return filled.reshape(SLOTS, BLOCK_LEN, -1, KV_HEADS, 2 * HEAD_DIM).astype(jnp.bfloat16)


def draw_queries(key, part):
    group_size = HEADS // KV_HEADS
    direction = sign_direction(key)
    head_dirs = jnp.repeat(direction, group_size, axis=0)
    mask_key, level_key, noise_key, fine_key = jax.random.split(jax.random.fold_in(key, 17), 4)
    drawn = jnp.clip(jax.random.normal(noise_key, (SLOTS, HEADS, HEAD_DIM), jnp.float32), -6.0, 6.0)
    picked = jax.random.bernoulli(mask_key, 0.25, (SLOTS, HEADS))
    strength = jax.random.uniform(level_key, (SLOTS, HEADS), jnp.float32, 2.2, 5.5)
    fine_noise = 0.1 * jnp.clip(jax.random.normal(fine_key, (SLOTS, HEADS, HEAD_DIM), jnp.float32), -3.0, 3.0)
    aligned = jnp.clip(strength[..., None] * head_dirs[None] + fine_noise, -6.0, 6.0)
    return jnp.where(picked[..., None], aligned, drawn).astype(jnp.bfloat16)


def set_ends(result, key, least, top_value):
    place = [jax.random.randint(jax.random.fold_in(key, axis), (), 0, length) for axis, length in enumerate(result.shape)]
    longest = result.shape.index(max(result.shape))
    neighbour = place[:longest] + [(place[longest] + 1) % result.shape[longest]] + place[longest + 1:]
    return result.at[tuple(place)].set(least).at[tuple(neighbour)].set(top_value)


def strengthened(drawn, own_key, source, target, parts, factor):
    def block_of(axis_at):
        return (jnp.arange(drawn.shape[axis_at]) // (drawn.shape[axis_at] // parts)).reshape((-1,) + (1,) * (drawn.ndim - 1 - axis_at))

    near = jax.random.permutation(own_key, parts)[block_of(target)]
    other_side = (block_of(target) + parts // 2) % parts
    return jnp.where((block_of(source) == near) | (block_of(source) == other_side), factor * drawn, drawn)


def block_scale(stream_key, extent, pieces, least, top_value):
    def one(dim, parts):
        draws = jax.random.uniform(jax.random.fold_in(jax.random.fold_in(stream_key, 6), dim), (parts,), jnp.float32, least / len(pieces), top_value / len(pieces))
        return jnp.repeat(jnp.exp(draws), extent[dim] // parts).reshape((-1,) + (1,) * (len(extent) - dim - 1))

    level = one(*pieces[0])
    for cut in pieces[1:]:
        level = level * one(*cut)
    return level


def gaussian(key, extent, width, reach, shards=(), held_as=jnp.bfloat16):
    drawn = jax.random.normal(key, extent, jnp.float32) * width
    if len(shards) > 0:
        drawn = block_scale(key, extent, shards, -0.22, 0.18) * drawn
    return jnp.clip(drawn, min=-reach, max=reach).astype(held_as)


def heavy_noise(own_key, extent, spread, bound, cuts, heavy, held_as=jnp.bfloat16):
    values = spread * jax.random.normal(own_key, extent, jnp.float32)
    if cuts:
        values = values * block_scale(own_key, extent, cuts, -0.22, 0.18)
    return jnp.clip(strengthened(values, jax.random.fold_in(own_key, 3), *heavy), -bound, bound).astype(held_as)


def setup_inputs(seed: int = 0, part: int = 0) -> dict:
    key_list = jax.random.split(jax.random.key(seed), 18)
    part_keys = jax.random.split(jax.random.fold_in(key_list[17], part), 18)
    prompt_cache = draw_prompt_cache(jax.random.fold_in(jax.random.fold_in(key_list[17], part), 71), part)
    prompt_states = heavy_noise(part_keys[1], (PROMPTS, N_SEQ, STATE, INNER), 1.0, 6.0, ((0, 2), (1, 8)), (1, 3, 8, 2.0), jnp.float32)
    block_steps = jnp.clip(jnp.exp(math.log(0.1) - 2.9957323 * jax.random.uniform(part_keys[2], (PROMPTS, N_SEQ, INNER), jnp.float32) ** block_scale(part_keys[2], (PROMPTS, N_SEQ, INNER), ((0, 2), (1, 8)), -0.2, 0.2)), 0.005, 0.1)
    prompt_lengths = set_ends(jax.random.randint(part_keys[3], (PROMPTS,), PROMPT_MAX // 6, PROMPT_MAX), jax.random.fold_in(part_keys[3], 1), PROMPT_MAX // 6, PROMPT_MAX - 1).astype(jnp.int32)
    target_slots = draw_target_slots(jax.random.fold_in(jax.random.fold_in(key_list[17], part), 71), part)
    cache_lengths = set_ends(jax.random.randint(part_keys[5], (SLOTS,), PROMPT_MAX // 6, PROMPT_MAX), jax.random.fold_in(part_keys[5], 1), PROMPT_MAX // 6, PROMPT_MAX - 1).astype(jnp.int32)
    resident_cache = draw_resident_cache(jax.random.fold_in(jax.random.fold_in(key_list[17], part), 71), part)
    token_cache = gaussian(part_keys[7], (SLOTS, KV_HEADS, 2 * HEAD_DIM), 1.0, 6.0, ((0, 2),))
    queries = draw_queries(jax.random.fold_in(jax.random.fold_in(key_list[17], part), 71), part)
    resident_states = gaussian(part_keys[9], (SLOTS, STATE, INNER), 1.0, 6.0, ((0, 2), (2, 8)), jnp.float32)
    decay_rates = jnp.clip(jnp.exp(jax.random.uniform(key_list[10], (STATE, INNER), jnp.float32, math.log(0.05), math.log(10.0))), 0.05, 10.0)
    step_sizes = jnp.clip(jnp.exp(math.log(1.0) - 4.6051702 * jax.random.uniform(part_keys[11], (SLOTS, INNER), jnp.float32) ** block_scale(part_keys[11], (SLOTS, INNER), ((0, 2), (1, 8)), -0.2, 0.2)), 0.01, 1.0)
    inner_input = gaussian(part_keys[12], (SLOTS, INNER), 1.0, 6.0, ((0, 2), (1, 8)))
    inner_gate = gaussian(part_keys[13], (SLOTS, INNER), 1.0, 6.0, ((0, 2), (1, 8)))
    state_input = gaussian(part_keys[14], (SLOTS, STATE), 1.0, 6.0, ((0, 2),), jnp.float32)
    state_readout = gaussian(part_keys[15], (SLOTS, STATE), 1.0, 6.0, ((0, 2),), jnp.float32)
    skip_gain = jnp.clip(0.5 + 1.0 * jax.random.uniform(key_list[16], (INNER,), jnp.float32) ** block_scale(key_list[16], (INNER,), ((0, 8),), -0.2, 0.2), 0.5, 1.5)
    return {"prompt_cache": prompt_cache, "prompt_states": prompt_states, "block_steps": block_steps, "prompt_lengths": prompt_lengths, "target_slots": target_slots, "cache_lengths": cache_lengths, "resident_cache": resident_cache, "token_cache": token_cache, "queries": queries, "resident_states": resident_states, "decay_rates": decay_rates, "step_sizes": step_sizes, "inner_input": inner_input, "inner_gate": inner_gate, "state_input": state_input, "state_readout": state_readout, "skip_gain": skip_gain}


def reference(prompt_cache, prompt_states, block_steps, prompt_lengths, target_slots, cache_lengths, resident_cache, token_cache, queries, resident_states, decay_rates, step_sizes, inner_input, inner_gate, state_input, state_readout, skip_gain):
    prompt_max = BLOCK_LEN * N_SEQ
    slot_count = SLOTS_DEV * N_BATCH
    kv_width = 2 * HEAD_DIM
    slot_ids = jnp.arange(slot_count, dtype=jnp.int32)
    matches = target_slots[None, :] == slot_ids[:, None]
    fresh = jnp.any(matches, axis=1)
    chosen_len = lax.optimization_barrier(jnp.sum(jnp.where(matches, prompt_lengths[None, :], 0), axis=1)).astype(jnp.int32)
    lengths = jnp.where(fresh, chosen_len, cache_lengths).astype(jnp.int32)
    picked = jnp.dot(matches.astype(jnp.bfloat16), prompt_cache.reshape(PROMPTS, -1), preferred_element_type=jnp.float32)
    picked = picked.astype(jnp.bfloat16).reshape(slot_count, prompt_max, KV_HEADS, kv_width)
    resident = resident_cache.reshape(slot_count, prompt_max, KV_HEADS, kv_width)
    position = jnp.arange(prompt_max, dtype=jnp.int32)
    merged = jnp.where(fresh[:, None, None, None], picked, resident)
    merged = jnp.where((position[None, :] < lengths[:, None])[:, :, None, None], merged, jnp.zeros((), jnp.bfloat16))
    merged = jnp.where((position[None, :] == lengths[:, None])[:, :, None, None], token_cache[:, None], merged)
    merged_cache = merged.reshape(slot_count, BLOCK_LEN, N_SEQ, KV_HEADS, kv_width)
    group = HEADS // KV_HEADS
    grouped = queries.reshape(slot_count, KV_HEADS, group, HEAD_DIM).astype(jnp.float32)
    scores = jnp.einsum('rgqd,rtgd->rgqt', grouped, merged[..., :HEAD_DIM].astype(jnp.float32)) * (1.0 / math.sqrt(HEAD_DIM))
    seen = (position[None, :] <= lengths[:, None])[:, None, None, :]
    masked = jnp.where(seen, scores, -1e+30)
    masked = masked.reshape(slot_count, KV_HEADS, group, BLOCK_LEN, N_SEQ)
    seen_cls = jnp.broadcast_to(seen, scores.shape).reshape(slot_count, KV_HEADS, group, BLOCK_LEN, N_SEQ)
    class_top = lax.optimization_barrier(jnp.max(masked, axis=3))
    weights = jnp.where(seen_cls, jnp.exp(masked - class_top[:, :, :, None, :]), 0.0)
    class_total = lax.optimization_barrier(jnp.sum(weights, axis=3))
    values = merged_cache[..., HEAD_DIM:].astype(jnp.float32)
    class_sum = jnp.einsum('rgqij,rijgd->rgqjd', weights.astype(jnp.bfloat16).astype(jnp.float32), values)
    overall = lax.optimization_barrier(jnp.max(class_top, axis=3))
    factor = jnp.exp(class_top - overall[..., None])
    total = lax.optimization_barrier(jnp.sum(class_total * factor, axis=3))
    summed = lax.optimization_barrier(jnp.sum(class_sum * factor[..., None], axis=3))
    attention = (summed / total[..., None]).reshape(slot_count, HEADS, HEAD_DIM).astype(jnp.bfloat16)
    starts = jnp.arange(N_SEQ, dtype=jnp.int32) * BLOCK_LEN
    usable = (starts[None, :] < prompt_lengths[:, None]).astype(jnp.float32)
    step_terms = block_steps * usable[:, :, None]
    later = lax.optimization_barrier(jnp.sum(step_terms, axis=1, keepdims=True)) - jnp.cumsum(step_terms, axis=1)

    def fold_prompt(packed):
        states, behind, weight = packed
        return lax.optimization_barrier(jnp.sum(weight[:, None, None] * jnp.exp(-decay_rates[None] * behind[:, None, :]) * states, axis=0))
    handed = lax.map(fold_prompt, (prompt_states, later, usable))
    chosen_state = jnp.einsum('rp,pnc->rnc', matches.astype(jnp.float32), handed, precision=lax.Precision.HIGHEST)
    start = jnp.where(fresh[:, None, None], chosen_state, resident_states)
    inner = inner_input.astype(jnp.float32)
    next_states = jnp.exp(-decay_rates[None] * step_sizes[:, None, :]) * start + (step_sizes * inner)[:, None, :] * state_input[:, :, None]
    readout = lax.optimization_barrier(jnp.sum(state_readout[:, :, None] * next_states, axis=1)) + skip_gain[None, :] * inner
    mamba_output = (readout * jax.nn.silu(inner_gate.astype(jnp.float32))).astype(jnp.bfloat16)
    return (merged_cache, attention, next_states, mamba_output)
```

```python
import functools
import math

import jax
import jax.numpy as jnp
from jax import lax
from jax.experimental import pallas as pl
from jax.experimental.pallas import tpu as pltpu
from jax.sharding import PartitionSpec as P

MESH = pl.DeviceIdType.MESH
FULL = 32760.0
LOW = -1e30


def kernel(
    dims,
    plen,
    tslot,
    clen,
    cache,
    states,
    steps,
    resident,
    token,
    queries,
    rstates,
    rates,
    dt,
    inner,
    gate,
    s_in,
    s_out,
    skip,
    merged,
    attention,
    nstates,
    mout,
    arrived,
    cache_send,
    handed,
    acc,
    osend,
    orecv,
    lse_send,
    lse_recv,
    *rest,
):
    n, nb, levels, block_len = dims
    d_send, d_recv, d_sel, d_cur, q_send, q_recv, m_send, m_recv = (
        rest[i * levels : (i + 1) * levels] for i in range(8)
    )
    (
        cache_ss, cache_rs, relay_ss, relay_rs, d_ss, d_rs, q_ss, q_rs, m_ss, m_rs,
        hand_ss, hand_rs, o_ss, o_rs, l_ss, l_rs,
    ) = rest[8 * levels :]
    me = lax.axis_index("seq")
    b = lax.axis_index("batch")
    prompts, rows, _, kv_heads, width = cache.shape
    all_prompts = prompts * nb
    requests, heads, head_dim = queries.shape
    state_n, channels = rates.shape
    share_len = channels // n
    chunk = min(512, share_len)
    per_share = share_len // chunk
    own_heads = heads // n
    group = heads // kv_heads
    positions = resident.shape[1]
    bits = [lax.rem(me // (1 << s), 2) for s in range(levels)]
    peers = [me + (1 - 2 * bits[s]) * (1 << s) for s in range(levels)]
    first = b * prompts

    def remote(src, dst, ss, rs, where):
        return pltpu.make_async_remote_copy(
            src_ref=src, dst_ref=dst, send_sem=ss, recv_sem=rs, device_id=where, device_id_type=MESH
        )

    barrier = pltpu.get_barrier_semaphore()
    for k in range(1, n):
        pl.semaphore_signal(
            barrier, inc=1, device_id={"seq": lax.rem(me + k, n)}, device_id_type=MESH
        )
    for k in range(1, nb):
        pl.semaphore_signal(
            barrier, inc=1, device_id={"batch": lax.rem(b + k, nb)}, device_id_type=MESH
        )
    pl.semaphore_wait(barrier, n - 1 + nb - 1)

    usable = [
        jnp.where(me * block_len < plen[first + p], 1.0, 0.0).astype(jnp.float32)
        for p in range(prompts)
    ]
    row_id = lax.broadcasted_iota(jnp.int32, (prompts, share_len), 0)
    usable_rows = jnp.zeros((prompts, share_len), jnp.float32)
    for p in range(prompts):
        usable_rows = jnp.where(row_id == p, usable[p], usable_rows)

    def lanes(share, c=0, size=share_len):
        return pl.ds(pl.multiple_of(share * share_len + c * chunk, 128), size)

    pending = []

    def start(copy):
        copy.start()
        pending.append(copy)
        return copy

    @pl.loop(0, n // 2)
    def _(k):
        d_send[0][k] = steps[:, lanes(2 * k + 1 - bits[0])] * usable_rows

    d_copies = [
        remote(
            d_send[s].at[pl.ds(0, n >> (s + 1))],
            d_recv[s].at[pl.ds(0, n >> (s + 1))],
            d_ss.at[s],
            d_rs.at[s],
            {"seq": peers[s]},
        )
        for s in range(levels)
    ]
    start(d_copies[0])

    @pl.loop(0, n)
    def _(to):
        cache_send[to] = cache[:, :, to]

    cache_copies = []
    for k in range(1, n):
        to = lax.rem(me + k, n)
        cache_copies.append(
            start(
                remote(
                    cache_send.at[to],
                    arrived.at[b, me],
                    cache_ss.at[k - 1],
                    cache_rs.at[k - 1],
                    {"seq": to},
                )
            )
        )
    arrived[b, me] = cache[:, :, me]

    def read(s, p, k, c):
        if s == 0:
            share = k
            return states[p, :, lanes(share, c, chunk)] * usable[p]
        return acc[p, k, :, pl.ds(pl.multiple_of(c * chunk, 128), chunk)]

    q_copies, m_copies = {}, {}

    def send_half(s, p):
        count = (n >> (s + 1)) * per_share

        def largest(i, top):
            k, c = i // per_share, lax.rem(i, per_share)
            return jnp.maximum(top, jnp.abs(read(s, p, 2 * k + 1 - bits[s], c)))

        top = lax.fori_loop(0, count, largest, jnp.full((state_n, chunk), 1e-30, jnp.float32))
        top = jnp.max(jnp.max(top, axis=0, keepdims=True), axis=1, keepdims=True)
        m_send[s][p] = jnp.broadcast_to(top, (8, 128))
        scale = FULL / top

        @pl.loop(0, count)
        def _(i):
            k, c = i // per_share, lax.rem(i, per_share)
            value = read(s, p, 2 * k + 1 - bits[s], c) * scale
            q_send[s][p, k, :, pl.ds(pl.multiple_of(c * chunk, 128), chunk)] = (
                jnp.round(value).astype(jnp.int32).astype(jnp.int16)
            )

        where = {"seq": peers[s]}
        m_copies[s, p] = start(
            remote(m_send[s].at[p], m_recv[s].at[p], m_ss.at[s, p], m_rs.at[s, p], where)
        )
        q_copies[s, p] = start(
            remote(q_send[s].at[p], q_recv[s].at[p], q_ss.at[s, p], q_rs.at[s, p], where)
        )

    for p in range(prompts):
        send_half(0, p)

    def fold_steps(s):
        d_copies[s].wait_recv()
        right = jnp.full((prompts, share_len), bits[s], jnp.int32) == 1

        @pl.loop(0, n >> (s + 1))
        def _(k):
            if s == 0:
                own = steps[:, lanes(2 * k + bits[0])] * usable_rows
            else:
                own = d_cur[s - 1][2 * k + bits[s]]
            other = d_recv[s][k]
            d_sel[s][k] = jnp.where(right, own, other)
            d_cur[s][k] = own + other

        if s + 1 < levels:

            @pl.loop(0, n >> (s + 2))
            def _(k):
                d_send[s + 1][k] = d_cur[s][2 * k + 1 - bits[s + 1]]

            start(d_copies[s + 1])

    fold_steps(0)

    for copy in cache_copies:
        copy.wait_recv()
    relays = []
    for k in range(1, nb):
        relays.append(
            start(
                remote(
                    arrived.at[b],
                    arrived.at[b],
                    relay_ss.at[k - 1],
                    relay_rs.at[k - 1],
                    {"batch": lax.rem(b + k, nb)},
                )
            )
        )
    for copy in relays:
        copy.wait_recv()

    def pick(r):
        slot = b * requests + r
        chosen, length, hits = jnp.int32(0), jnp.int32(0), jnp.int32(0)
        for p in range(all_prompts):
            hit = tslot[p] == slot
            chosen = jnp.where(hit, p, chosen)
            length = jnp.where(hit, plen[p], length)
            hits = jnp.where(hit, 1, hits)
        return chosen, hits, jnp.where(hits > 0, length, clen[r])

    shape3 = (positions, kv_heads, width)
    position = lax.broadcasted_iota(jnp.int32, shape3, 0) * n + me
    flat = positions * kv_heads
    column = lax.broadcasted_iota(jnp.int32, (heads, flat), 1)
    owner = lax.broadcasted_iota(jnp.int32, (heads, flat), 0) // group
    same_head = lax.rem(column, kv_heads) == owner
    column_position = (column // kv_heads) * n + me
    lane_id = lax.broadcasted_iota(jnp.int32, (heads, 128), 1)

    def attend(r, lse_all):
        chosen, hits, length = pick(r)
        fresh_limit = jnp.where(hits > 0, length, 0)
        new = arrived[chosen // prompts, :, lax.rem(chosen, prompts)].reshape(shape3).astype(jnp.float32)
        old = resident[r].astype(jnp.float32)
        x = jnp.where(position < fresh_limit, new, old)
        x = jnp.where(position < length, x, 0.0)
        x = jnp.where(position == length, token[r].astype(jnp.float32)[None], x)
        merged[r] = x.astype(jnp.bfloat16)
        x2 = x.reshape(flat, width)
        keys = x2[:, :head_dim].astype(jnp.bfloat16)
        values = x2[:, head_dim:].astype(jnp.bfloat16)
        score = lax.dot_general(
            queries[r], keys, (((1,), (1,)), ((), ())), preferred_element_type=jnp.float32
        ) * (1.0 / math.sqrt(head_dim))
        seen = same_head & (column_position <= length)
        score = jnp.where(seen, score, LOW)
        top = jnp.max(score, axis=1, keepdims=True)
        weight = jnp.where(seen, jnp.exp(score - top), 0.0)
        total = jnp.sum(weight, axis=1, keepdims=True)
        out = jnp.dot(weight.astype(jnp.bfloat16), values, preferred_element_type=jnp.float32)
        some = total > 0.0
        safe = jnp.where(some, total, 1.0)
        out = out / safe
        lse = jnp.where(some, top + jnp.log(safe), LOW)
        for j in range(n):
            osend[j, r] = out[j * own_heads : (j + 1) * own_heads]
        return jnp.where(lane_id == r, lse, lse_all)

    lse_all = lax.fori_loop(0, requests, attend, jnp.zeros((heads, 128), jnp.float32))
    for j in range(n):
        lse_send[j] = lse_all[j * own_heads : (j + 1) * own_heads]
    o_copies = []
    for k in range(1, n):
        to = lax.rem(me + k, n)
        o_copies.append(
            start(
                remote(
                    lse_send.at[to], lse_recv.at[me], l_ss.at[k - 1], l_rs.at[k - 1], {"seq": to}
                )
            )
        )
        o_copies.append(
            start(
                remote(osend.at[to], orecv.at[me], o_ss.at[k - 1], o_rs.at[k - 1], {"seq": to})
            )
        )
    lse_recv[me] = lse_send[me]
    orecv[me] = osend[me]

    for s in range(1, levels):
        fold_steps(s)

    hand_copies = []

    def fold(s, p):
        m_copies[s, p].wait_recv()
        q_copies[s, p].wait_recv()
        scale = m_recv[s][p][0:1, 0:1] * (1.0 / FULL)
        right = jnp.full((state_n, chunk), bits[s], jnp.int32) == 1
        below = lax.rem(me, 1 << (s + 1))

        @pl.loop(0, (n >> (s + 1)) * per_share)
        def _(i):
            k, c = i // per_share, lax.rem(i, per_share)
            at = pl.ds(pl.multiple_of(c * chunk, 128), chunk)
            other = q_recv[s][p, k, :, at].astype(jnp.int32).astype(jnp.float32) * scale
            own = read(s, p, 2 * k + bits[s], c)
            rate = rates[:, lanes(k * (1 << (s + 1)) + below, c, chunk)]
            decay = jnp.exp(-rate * d_sel[s][k, :, at][p : p + 1])
            early = jnp.where(right, other, own)
            late = jnp.where(right, own, other)
            folded = decay * early + late
            if s + 1 < levels:
                acc[p, k, :, at] = folded
            else:
                handed[first + p, :, at] = folded

        if s + 1 < levels:
            send_half(s + 1, p)
        else:
            for k in range(1, nb):
                hand_copies.append(
                    start(
                        remote(
                            handed.at[first + p],
                            handed.at[first + p],
                            hand_ss.at[k - 1, p],
                            hand_rs.at[k - 1, p],
                            {"batch": lax.rem(b + k, nb)},
                        )
                    )
                )

    for wave in range(prompts + levels - 1):
        for s in reversed(range(levels)):
            p = wave - s
            if 0 <= p < prompts:
                fold(s, p)

    for copy in o_copies:
        copy.wait_recv()
    lane3 = lax.broadcasted_iota(jnp.int32, (n, own_heads, 128), 2)
    for r in range(requests):
        lse = jnp.sum(jnp.where(lane3 == r, lse_recv[...], 0.0), axis=2, keepdims=True)
        share = jnp.exp(lse - jnp.max(lse, axis=0, keepdims=True))
        top = jnp.sum(share * orecv[:, r], axis=0)
        attention[r] = (top / jnp.sum(share, axis=0)).astype(jnp.bfloat16)

    for copy in hand_copies:
        copy.wait_recv()

    eye = lax.broadcasted_iota(jnp.int32, (state_n, state_n), 0) == lax.broadcasted_iota(
        jnp.int32, (state_n, state_n), 1
    )

    def as_column(row):
        spread = jnp.where(eye, jnp.broadcast_to(row, (state_n, state_n)), 0.0)
        return jnp.sum(spread, axis=1, keepdims=True)

    picks = [pick(r) for r in range(requests)]
    in_all, out_all = s_in[...], s_out[...]
    in_cols = [as_column(in_all[r : r + 1]) for r in range(requests)]
    out_cols = [as_column(out_all[r : r + 1]) for r in range(requests)]

    @pl.loop(0, per_share)
    def _(c):
        at = pl.ds(pl.multiple_of(c * chunk, 128), chunk)
        step_rows = dt[:, at]
        x_rows = inner[:, at].astype(jnp.float32)
        g = gate[:, at].astype(jnp.float32)
        rate = -rates[:, lanes(me, c, chunk)]
        push_rows = step_rows * x_rows
        out_rows = []
        for r in range(requests):
            chosen, hits, _ = picks[r]
            fresh = jnp.full((state_n, chunk), hits, jnp.int32) > 0
            begin = jnp.where(fresh, handed[chosen, :, at], rstates[r, :, at])
            after = jnp.exp(rate * step_rows[r : r + 1]) * begin
            after = after + push_rows[r : r + 1] * in_cols[r]
            nstates[r, :, at] = after
            out_rows.append(jnp.sum(out_cols[r] * after, axis=0, keepdims=True))
        read_out = jnp.concatenate(out_rows, axis=0) + skip[:, at] * x_rows
        mout[:, at] = (read_out * (g / (1.0 + jnp.exp(-g)))).astype(jnp.bfloat16)

    for copy in pending:
        copy.wait_send()


def local(
    n,
    nb,
    prompt_cache,
    prompt_states,
    block_steps,
    prompt_lengths,
    target_slots,
    cache_lengths,
    resident_cache,
    token_cache,
    queries,
    resident_states,
    decay_rates,
    step_sizes,
    inner_input,
    inner_gate,
    state_input,
    state_readout,
    skip_gain,
):
    levels = n.bit_length() - 1
    prompts, block_len, kv_heads, width = prompt_cache.shape
    requests, heads, head_dim = queries.shape
    state_n, channels = decay_rates.shape
    share = channels // n
    own_heads = heads // n
    positions = resident_cache.shape[1]
    all_prompts = prompts * nb
    f32, bf16, i16 = jnp.float32, jnp.bfloat16, jnp.int16
    vmem = pl.BlockSpec(memory_space=pltpu.VMEM)
    smem = pl.BlockSpec(memory_space=pltpu.SMEM)
    dma = pltpu.SemaphoreType.DMA
    halves = [n >> (s + 1) for s in range(levels)]
    scratch = [
        pltpu.VMEM((nb, n, prompts, block_len // n, kv_heads, width), bf16),
        pltpu.VMEM((n, prompts, block_len // n, kv_heads, width), bf16),
        pltpu.VMEM((all_prompts, state_n, share), f32),
        pltpu.VMEM((prompts, n // 2, state_n, share), f32),
        pltpu.VMEM((n, requests, own_heads, head_dim), f32),
        pltpu.VMEM((n, requests, own_heads, head_dim), f32),
        pltpu.VMEM((n, own_heads, 128), f32),
        pltpu.VMEM((n, own_heads, 128), f32),
    ]
    for _ in range(4):
        scratch += [pltpu.VMEM((h + 1, prompts, share), f32) for h in halves]
    for _ in range(2):
        scratch += [pltpu.VMEM((prompts, h, state_n, share), i16) for h in halves]
    for _ in range(2):
        scratch += [pltpu.VMEM((prompts, 8, 128), f32) for h in halves]
    scratch += [dma((n - 1,))] * 2
    scratch += [dma((max(nb - 1, 1),))] * 2
    scratch += [dma((levels,))] * 2
    scratch += [dma((levels, prompts))] * 4
    scratch += [dma((max(nb - 1, 1), prompts))] * 2
    scratch += [dma((n - 1,))] * 4
    merged, attention, next_states, mamba_output = pl.pallas_call(
        functools.partial(kernel, (n, nb, levels, block_len)),
        out_shape=(
            jax.ShapeDtypeStruct((requests, positions, kv_heads, width), bf16),
            jax.ShapeDtypeStruct((requests, own_heads, head_dim), bf16),
            jax.ShapeDtypeStruct((requests, state_n, share), f32),
            jax.ShapeDtypeStruct((requests, share), bf16),
        ),
        in_specs=[smem] * 3 + [vmem] * 14,
        out_specs=(vmem,) * 4,
        scratch_shapes=scratch,
        compiler_params=pltpu.CompilerParams(
            collective_id=0, has_side_effects=True, vmem_limit_bytes=48 << 20
        ),
    )(
        prompt_lengths,
        target_slots,
        cache_lengths,
        prompt_cache.reshape(prompts, block_len // n, n, kv_heads, width),
        prompt_states[:, 0],
        block_steps[:, 0],
        resident_cache[:, :, 0],
        token_cache,
        queries,
        resident_states,
        decay_rates,
        step_sizes,
        inner_input,
        inner_gate,
        state_input,
        state_readout,
        skip_gain[None],
    )
    return merged[:, :, None], attention, next_states, mamba_output


def solution(mesh):
    n, nb = mesh.shape["seq"], mesh.shape["batch"]
    return jax.shard_map(
        functools.partial(local, n, nb),
        mesh=mesh,
        in_specs=(
            P(("groups", "batch"), "seq", None, None),
            P(("groups", "batch"), "seq", None, None),
            P(("groups", "batch"), "seq", None),
            P("groups"),
            P("groups"),
            P(("groups", "batch")),
            P(("groups", "batch"), None, "seq", None, None),
            P(("groups", "batch"), None, None),
            P(("groups", "batch"), None, None),
            P(("groups", "batch"), None, "seq"),
            P(),
            P(("groups", "batch"), "seq"),
            P(("groups", "batch"), "seq"),
            P(("groups", "batch"), "seq"),
            P(("groups", "batch"), None),
            P(("groups", "batch"), None),
            P("seq"),
        ),
        out_specs=(
            P(("groups", "batch"), None, "seq", None, None),
            P(("groups", "batch"), "seq", None),
            P(("groups", "batch"), None, "seq"),
            P(("groups", "batch"), "seq"),
        ),
        check_vma=False,
    )
```
